32 devices in a mesh: gx: 8 (over y, x, core), gy: 4 (over z).
Axes of the slice: x: 2, y: 2, z: 4, core: 2. Of those that a mesh axis runs over, the one named last changes fastest.
Arguments:
- point_feats: bfloat16 [262144, 128], P(('gx', 'gy')), may hold values from -6 to 6
- point_tile: int32 [262144, 1], P(('gx', 'gy')), may hold values from 0 to 31; in each aligned block of 8192 rows (0 to 8191, 8192 to 16383, ...) at most 320 rows name the same one
- point_cell: int32 [262144], P(('gx', 'gy')), may hold values from 0 to 4095
- point_count: int32 [32], P(('gx', 'gy')), may hold values from 6144 to 8192, as said below
- conv_weight: bfloat16 [3, 3, 128, 128], replicated, may hold values from -0.1875 to 0.1875
- conv_bias: float32 [128], replicated, may hold values from -3 to 3
Outputs:
- bev_map: bfloat16 [128, 1024, 128], P('gx', 'gy')
- conv_out: bfloat16 [128, 1024, 128], P('gx', 'gy')
The draws below stay inside these ranges and needn't reach their ends.
Inputs may be any that keep to these rules, and one draw needn't show every extreme that they name: `point_tile`: among the 8192 rows of one device no tile is named by more than 320 rows, a bound that some block reaches. `point_count`: only slots below a device's count are live; some device has all 8192 slots live.
All inputs are finite; a program needn't handle non-finite values.
Results may differ from the reference program's by a relative error of at most 0.0045.
Values may be sent and summed in bfloat16 or wider, within the bound.
A program may use at most 64 MiB of HBM per device.

```python
import math
import jax
import jax.numpy as jnp
import numpy as np
from jax import lax

C = 128
COLS_DEV = 256
ROWS_DEV = 16
P_DEV = 8192
CAP = 320
POINTS = 262144
MAP_ROWS = 128
MAP_COLS = 1024
N_GY = 4
DEVICES = 32


def draw_point_count(key, part):
    counts = jax.random.randint(key, (DEVICES,), 3 * P_DEV // 4, P_DEV + 1).astype(jnp.int32)
    fullest = jax.random.randint(jax.random.fold_in(key, 7), (), 0, DEVICES)
    return counts.at[fullest].set(P_DEV)


def with_ends(array, key, low, high):
    longest = array.shape.index(max(array.shape))
    spots = []
    for shift in (0, 1):
        where = [jax.random.randint(jax.random.fold_in(key, axis), (), 0, length) for axis, length in enumerate(array.shape)]
        where[longest] = (where[longest] + shift) % array.shape[longest]
        spots.append(tuple(where))
    return array.at[spots[0]].set(low).at[spots[1]].set(high)


def level_of(own_key, dims, cuts, low, largest):
    loudness, own = 1.0, jax.random.fold_in(own_key, 6)
    for dim, blocks in cuts:
        steps = jnp.exp(jax.random.uniform(jax.random.fold_in(own, dim), (blocks,), jnp.float32, low / len(cuts), largest / len(cuts)))
        loudness = loudness * jnp.repeat(steps, dims[dim] // blocks).reshape([-1 if axis == dim else 1 for axis in range(len(dims))])
    return loudness


def routed_block(own_key, own, number, rows, count, top, most, slope):
    sequence = jax.random.permutation(own_key, count)
    packed, usual = load_shares(count, rows * top, most, slope, True), load_shares(count, rows * top, most, slope, False)
    places = jnp.arange(count)

    def named(lengths, rotation):
        used = int((lengths > 0).sum())
        fixed = max(1, used // 4)
        passed = fixed + (places - fixed + rotation * (used - fixed)) % max(1, count - fixed)
        return jnp.zeros((count,), jnp.int32).at[sequence[jnp.where(places < fixed, places, passed)]].set(jnp.asarray(lengths, jnp.int32))

    lengths = jnp.where(number % 4 == 0, named(packed, number // 4), named(usual, number - number // 4 - 1))
    mixed = jax.random.permutation(jax.random.fold_in(own, 3), count)
    source_of, sink = mixed[0:count // 2 * 2:2], mixed[1:count // 2 * 2:2]
    margin = jnp.minimum(lengths[source_of] - 1, most - lengths[sink]) // 2
    margin = jnp.where((source_of == sequence[0]) | (sink == sequence[0]) | (lengths[sink] == 0), 0, jnp.maximum(margin, 0))
    passed = jax.random.randint(jax.random.fold_in(own, 4), (count // 2,), 0, 1 << 20) % (margin + 1)
    lengths = lengths.at[source_of].add(-passed).at[sink].add(passed)
    labels = jnp.searchsorted(jnp.cumsum(lengths), jnp.arange(rows * top), side="right").astype(jnp.int32)
    grid = labels.reshape(top, rows).T
    grid = grid[jax.random.permutation(jax.random.fold_in(own, 1), rows)]
    rotation = jax.random.randint(jax.random.fold_in(own, 2), (rows, 1), 0, top)
    return jnp.take_along_axis(grid, (jnp.arange(top)[None, :] + rotation) % top, axis=1)


def load_shares(number_of, total, bound, lean, full):
    loads = [(1 << 20) // math.isqrt(grade ** lean) + 1 for grade in range(1, number_of + 1)]
    largest = bound if full else min(bound, max(-(-total // number_of), total * loads[0] // sum(loads)))
    least = 1 if total - largest >= number_of - 1 else 0
    holding, spare = [largest] + [least] * (number_of - 1), total - largest - least * (number_of - 1)
    while spare > 0:
        candidates = [i for i in range(1, number_of) if holding[i] < largest] or [i for i in range(1, number_of) if holding[i] < bound]
        pool, left = sum([loads[i] for i in candidates]), spare
        for i in candidates:
            more = min(bound - holding[i], max(1, left * loads[i] // pool), spare)
            holding[i] = holding[i] + more
            spare = spare - more
    return np.array(holding)


def scatter_about(own_key, dims, deviation, reach, cuts=(), kind=jnp.bfloat16):
    drawn = jax.random.normal(own_key, dims, jnp.float32) * deviation
    if len(cuts) > 0:
        drawn = level_of(own_key, dims, cuts, -0.22, 0.18) * drawn
    return jnp.clip(drawn, min=-reach, max=reach).astype(kind)


def setup_inputs(seed: int = 0) -> dict:
    seeds = jax.random.split(jax.random.key(seed), 7)
    point_feats = scatter_about(seeds[0], (POINTS, C), 1.0, 6.0, ((0, 32),))
    point_tile_keys = jax.random.split(jax.random.fold_in(seeds[1], 1), POINTS // P_DEV)
    point_tile_turns = jax.random.permutation(jax.random.fold_in(seeds[1], 3), POINTS // P_DEV)
    point_tile = jax.vmap(lambda own, number: routed_block(jax.random.fold_in(seeds[1], 2), own, number, P_DEV, DEVICES, 1, CAP, 2))(point_tile_keys, point_tile_turns).reshape((POINTS, 1))
    point_cell = with_ends(jax.random.randint(seeds[2], (POINTS,), 0, ROWS_DEV * COLS_DEV), jax.random.fold_in(seeds[2], 1), 0, (ROWS_DEV * COLS_DEV) - 1).astype(jnp.int32)
    point_count = draw_point_count(jax.random.fold_in(seeds[6], 71), 0)
    conv_weight = scatter_about(seeds[4], (3, 3, C, C), (9 * C) ** -0.5, 0.1875)
    conv_bias = scatter_about(seeds[5], (C,), 0.5, 3.0, (), jnp.float32)
    return dict(point_feats=point_feats, point_tile=point_tile, point_cell=point_cell, point_count=point_count, conv_weight=conv_weight, conv_bias=conv_bias)


def reference(point_feats, point_tile, point_cell, point_count, conv_weight, conv_bias):
    tile = point_tile[:, 0]
    rows = (tile // N_GY) * ROWS_DEV + point_cell // COLS_DEV
    cols = (tile % N_GY) * COLS_DEV + point_cell % COLS_DEV
    cell = rows * MAP_COLS + cols
    slot = jnp.arange(POINTS, dtype=jnp.int32)
    block = slot // P_DEV
    live = (slot % P_DEV) < point_count[block]
    feats = jnp.where(live[:, None], point_feats.astype(jnp.float32), 0.0)
    sums = jax.ops.segment_sum(feats, cell, num_segments=MAP_ROWS * MAP_COLS)
    bev_map = sums.reshape(MAP_ROWS, MAP_COLS, C).astype(jnp.bfloat16)
    conv = lax.conv_general_dilated(bev_map.astype(jnp.float32)[None], conv_weight.astype(jnp.float32), (1, 1), "SAME", dimension_numbers=("NHWC", "HWIO", "NHWC"), precision=lax.Precision.HIGHEST)[0]
    conv_out = jax.nn.relu(conv + conv_bias).astype(jnp.bfloat16)
    return bev_map, conv_out
```

```python
import functools

import jax
import jax.numpy as jnp
from jax import lax
from jax.experimental import pallas as pl
from jax.experimental.pallas import tpu as pltpu
from jax.sharding import PartitionSpec as P

COLS_DEV = 256
ROWS_DEV = 16
CELLS = ROWS_DEV * COLS_DEV


MESH = pl.DeviceIdType.MESH
GROUP = 4
CHUNK = 1024
NEIGHBOURS = [(dx, dy) for dx in (-1, 0, 1) for dy in (-1, 0, 1) if (dx, dy) != (0, 0)]


def map_kernel(
    size_gx,
    size_gy,
    count,
    source,
    named,
    cell,
    taps,
    bias,
    bev,
    conv,
    weight,
    feats,
    slots,
    tiles,
    meta,
    send_feats,
    send_cells,
    got_feats,
    got_cells,
    acc,
    pad,
    edges,
    sides,
    ends,
    flat,
    fetch,
    send_f,
    recv_f,
    send_c,
    recv_c,
    own,
    send_h,
    recv_h,
):
    devices = size_gx * size_gy
    capacity = send_feats.shape[1]
    gx, gy = lax.axis_index("gx"), lax.axis_index("gy")
    me = gx * size_gy + gy

    barrier = pltpu.get_barrier_semaphore()

    @pl.loop(1, devices)
    def _(k):
        other = lax.rem(me + k, devices)
        pl.semaphore_signal(
            barrier, inc=1, device_id=(other // size_gy, lax.rem(other, size_gy)), device_id_type=MESH
        )

    load = pltpu.make_async_copy(source, feats, fetch.at[0])
    load.start()

    for r in (0, ROWS_DEV + 1):
        pad[r] = jnp.zeros_like(pad[r])
    sides[...] = jnp.zeros_like(sides)

    chunks = named.shape[0]

    inner = 256
    upper = lax.broadcasted_iota(jnp.int32, (inner, inner), 0) <= lax.broadcasted_iota(
        jnp.int32, (inner, inner), 1
    )
    upper = jnp.where(upper, 1.0, 0.0).astype(jnp.bfloat16)
    names = lax.broadcasted_iota(jnp.int32, (devices, inner), 0)

    def prepare(c, before):
        slot = lax.broadcasted_iota(jnp.int32, (1, CHUNK), 1) + c * CHUNK
        target = jnp.where(slot < count[0], named[c], devices)
        hits = jnp.concatenate(
            [jnp.where(names == target[:, at : at + inner], 1.0, 0.0) for at in range(0, CHUNK, inner)],
            axis=0,
        )
        ranks = jnp.dot(hits.astype(jnp.bfloat16), upper, preferred_element_type=jnp.float32)
        found = []
        for at in range(0, CHUNK // inner * devices, devices):
            hit, rank = hits[at : at + devices], ranks[at : at + devices]
            found.append(jnp.sum(hit * (rank + before), axis=0, keepdims=True) - 1.0)
            before = before + rank[:, inner - 1 : inner]
        place = jnp.concatenate(found, axis=1).astype(jnp.int32)
        rows = pl.ds(pl.multiple_of(c * CHUNK, CHUNK), CHUNK)
        ids = lax.broadcasted_iota(jnp.int32, (capacity, CHUNK), 0)
        slots[c] = jnp.where(ids == place, 1.0, 0.0).astype(jnp.bfloat16)
        key = (target * CELLS + cell[c]).astype(jnp.float32)
        key = jnp.transpose(jnp.broadcast_to(key, (128, CHUNK))).astype(jnp.int32)
        tile = jnp.right_shift(key, 12)
        tiles[rows, :] = tile.astype(jnp.float32).astype(jnp.bfloat16)
        hit = tile == lax.broadcasted_iota(jnp.int32, (CHUNK, 128), 1)
        row = (jnp.right_shift(key, 8) & (ROWS_DEV - 1)) + 1
        col = key & (COLS_DEV - 1)
        for at, part in ((0, row), (128, col)):
            part = jnp.where(hit, part, 0).astype(jnp.float32)
            meta[rows, at : at + 128] = part.astype(jnp.bfloat16)
        return before

    lax.fori_loop(0, chunks, prepare, jnp.zeros((devices, inner), jnp.float32))

    def packed(operand):
        total = None
        for c in range(chunks):
            part = jnp.dot(slots[c], operand(c), preferred_element_type=jnp.float32)
            total = part if total is None else total + part
        return total

    def copies(source, owner, target):
        where = dict(
            device_id=(target // size_gy, lax.rem(target, size_gy)), device_id_type=MESH
        )
        return (
            pltpu.make_async_remote_copy(
                send_cells.at[source], got_cells.at[owner],
                send_c.at[source], recv_c.at[owner], **where,
            ),
            pltpu.make_async_remote_copy(
                send_feats.at[source], got_feats.at[owner], send_f.at[source], recv_f.at[owner], **where
            ),
        )

    mine = (
        pltpu.make_async_copy(send_cells.at[me], got_cells.at[me], own.at[0]),
        pltpu.make_async_copy(send_feats.at[me], got_feats.at[me], own.at[1]),
    )
    pairs = devices // 2
    half = me // 2

    def offset(q):
        return lax.rem(2 * q + 1, pairs) - q // (pairs // 2)

    def pack(q):
        pair = lax.rem(half + offset(q), pairs)
        names = [(pair * 2 + k).astype(jnp.float32).astype(jnp.bfloat16) for k in range(2)]

        def masked(c):
            rows = slice(c * CHUNK, (c + 1) * CHUNK)
            values, tile = feats[rows, :], tiles[rows, :]
            zero = jnp.zeros_like(values)
            return jnp.concatenate([jnp.where(tile == n, values, zero) for n in names], axis=1)

        block = packed(masked).astype(jnp.bfloat16)
        for k in range(2):
            send_feats[pair * 2 + k] = block[:, k * 128 : (k + 1) * 128]

    def send(q):
        pair = lax.rem(half + offset(q), pairs)
        for k in range(2):
            target = pair * 2 + k

            @pl.when(target != me)
            def _():
                for copy in copies(target, me, target):
                    copy.start()

            @pl.when(target == me)
            def _():
                for copy in mine:
                    copy.start()

    load.wait()
    pack(jnp.int32(0))

    found = packed(lambda c: meta[c * CHUNK : (c + 1) * CHUNK, :])
    found = found[:, :128] * 256.0 + found[:, 128:]
    if send_cells.shape[2] > capacity:
        found = jnp.concatenate(
            [found, jnp.zeros((send_cells.shape[2] - capacity, 128), jnp.float32)], axis=0
        )
    found = jnp.transpose(found)
    for t in range(devices):
        send_cells[t] = found[t : t + 1, :]

    pl.semaphore_wait(barrier, devices - 1)
    send(jnp.int32(0))

    @pl.loop(1, pairs)
    def _(q):
        pack(q)

        @pl.when(q > 1)
        def _():
            send(q - 1)

    for a in range(3):
        for b in range(3):
            weight[a * 128 : (a + 1) * 128, b * 128 : (b + 1) * 128] = taps[a, b]
    send(jnp.int32(pairs - 1))
    acc[...] = jnp.zeros_like(acc)

    def receive(positions):
        owners = []
        for j in positions:
            q = lax.rem(j + pairs // 2, pairs)
            pair = lax.rem(half + pairs - offset(q), pairs)
            owners += [pair * 2, pair * 2 + 1]
        for owner in owners:

            @pl.when(owner != me)
            def _():
                for copy in copies(owner, owner, owner):
                    copy.wait_recv()

            @pl.when(owner == me)
            def _():
                for copy in mine:
                    copy.wait()

        cells = [got_cells[owner] for owner in owners]
        values = jnp.concatenate([got_feats[owner] for owner in owners], axis=0)
        row, onehot = [], []
        for part in cells:
            part = part.astype(jnp.int32)
            at = (jnp.right_shift(part, 8) - 1).astype(jnp.float32)
            at = jnp.transpose(jnp.broadcast_to(at, (128, part.shape[1])))
            row.append(at[:capacity].astype(jnp.bfloat16))
            part = part[:, :capacity]
            onehot.append(part & (COLS_DEV - 1))
        row = jnp.concatenate(row, axis=0)
        col = jnp.concatenate(onehot, axis=1)
        ids = lax.broadcasted_iota(jnp.int32, (COLS_DEV, col.shape[1]), 0)
        onehot = jnp.where(ids == col, 1.0, 0.0).astype(jnp.bfloat16)
        zero = jnp.zeros_like(values)

        def added(rows):
            masked = jnp.concatenate(
                [jnp.where(row == jnp.bfloat16(r), values, zero) for r in rows], axis=1
            )
            return jnp.dot(onehot, masked, preferred_element_type=jnp.float32)

        return added

    group = GROUP // 2

    @pl.loop(0, pairs // group - 1)
    def _(g):
        added = receive([g * group + j for j in range(group)])
        for r in range(0, ROWS_DEV, 2):
            acc[:, r * 128 : (r + 2) * 128] += added((r, r + 1))

    for j in range(pairs - group, pairs - 1):
        added = receive([jnp.int32(j)])
        for r in range(0, ROWS_DEV, 2):
            acc[:, r * 128 : (r + 2) * 128] += added((r, r + 1))

    def inside(x, y):
        return (x >= 0) & (x < size_gx) & (y >= 0) & (y < size_gy)

    def halo(i):
        dx, dy = NEIGHBOURS[i]
        if dy == 0:
            src, dst = (pad.at[1], pad.at[ROWS_DEV + 1]) if dx < 0 else (pad.at[ROWS_DEV], pad.at[0])
        else:
            from_side, to_side = (0, 1) if dy < 0 else (1, 0)
            if dx == 0:
                src = edges.at[from_side]
                dst = sides.at[to_side, pl.ds(1, ROWS_DEV)]
            else:
                at = 0 if dx < 0 else ROWS_DEV - 1
                src = edges.at[from_side, pl.ds(at, 1)]
                dst = sides.at[to_side, pl.ds(ROWS_DEV + 1 if dx < 0 else 0, 1)]
        return pltpu.make_async_remote_copy(
            src, dst, send_h.at[i], recv_h.at[i], device_id=(gx + dx, gy + dy), device_id_type=MESH
        )

    def start(which):
        for i, (dx, dy) in enumerate(NEIGHBOURS):
            if which(dx, dy):

                @pl.when(inside(gx + dx, gy + dy))
                def _():
                    halo(i).start()

    added = receive([jnp.int32(pairs - 1)])
    order = [(0, ROWS_DEV - 1)] + [(r, r + 1) for r in range(1, ROWS_DEV - 1, 2)]
    for step, rows in enumerate(order):
        part = added(rows)
        for k, r in enumerate(rows):
            total = acc[:, r * 128 : (r + 1) * 128] + part[:, k * 128 : (k + 1) * 128]
            cells = total.astype(jnp.bfloat16)
            pad[r + 1] = cells
            bev[r] = cells
            for side, c in ((0, 0), (1, COLS_DEV - 1)):
                edges[side, r] = total[c : c + 1].astype(jnp.bfloat16).astype(jnp.float32)
        if step == 1:
            start(lambda dx, dy: dy == 0)
        if step == 2:
            start(lambda dx, dy: dx != 0 and dy != 0)

    place = lax.broadcasted_iota(jnp.int32, (COLS_DEV, 128), 0)

    def sums_of(r):
        near = jnp.concatenate([pad[r + a] for a in range(3)], axis=1)
        sums = jnp.dot(near, weight[...], preferred_element_type=jnp.float32)
        left = jnp.where(place == 0, 0.0, pltpu.roll(sums[:, :128], 1, 0))
        right = jnp.where(place == COLS_DEV - 1, 0.0, pltpu.roll(sums[:, 256:], COLS_DEV - 1, 0))
        total = sums[:, 128:256] + left + right + bias[...]
        for side, c in ((0, 0), (1, COLS_DEV - 1)):
            ends[side, r] = total[c : c + 1]
        conv[r] = jnp.maximum(total, 0.0).astype(jnp.bfloat16)

    start(lambda dx, dy: dx == 0)

    @pl.loop(1, ROWS_DEV - 1)
    def _(r):
        sums_of(r)

    for i, (dx, dy) in enumerate(NEIGHBOURS):

        @pl.when(inside(gx - dx, gy - dy))
        def _():
            halo(i).wait_recv()

    for r in (0, ROWS_DEV - 1):
        sums_of(r)

    side_sums = []
    for side in range(2):
        for r in range(ROWS_DEV + 2):
            flat[r : r + 1, :] = sides[side, r]
        near = jnp.concatenate([flat[a : a + ROWS_DEV, :] for a in range(3)], axis=1)
        part = weight[:, :128] if side == 0 else weight[:, 256:]
        side_sums.append(
            jnp.dot(near.astype(jnp.bfloat16), part, preferred_element_type=jnp.float32)
        )
    lines = 16
    place = lax.broadcasted_iota(jnp.int32, (lines, 128), 0)
    for side, c in ((0, 0), (1, COLS_DEV - 1)):
        rows = pl.ds(c // lines * lines, lines)
        for r in range(ROWS_DEV):
            total = jnp.maximum(ends[side, r] + side_sums[side][r : r + 1], 0.0)
            kept = conv[r, rows, :].astype(jnp.float32)
            conv[r, rows, :] = jnp.where(place == c % lines, total, kept).astype(jnp.bfloat16)

    for i, (dx, dy) in enumerate(NEIGHBOURS):

        @pl.when(inside(gx + dx, gy + dy))
        def _():
            halo(i).wait_send()

    @pl.loop(1, devices)
    def _(k):
        other = lax.rem(me + k, devices)
        for copy in copies(other, me, other):
            copy.wait_send()


def make_map(count, feats, named, cell, weight, bias, size_gx, size_gy, capacity):
    devices = size_gx * size_gy
    points, channels = feats.shape
    stride = -(-capacity // 128) * 128
    vmem = pl.BlockSpec(memory_space=pltpu.VMEM)
    shape = jax.ShapeDtypeStruct((ROWS_DEV, COLS_DEV, channels), jnp.bfloat16)
    dma = pltpu.SemaphoreType.DMA
    return pl.pallas_call(
        functools.partial(map_kernel, size_gx, size_gy),
        out_shape=(shape, shape),
        in_specs=[
            pl.BlockSpec(memory_space=pltpu.SMEM),
            pl.BlockSpec(memory_space=pltpu.HBM),
            vmem,
            vmem,
            vmem,
            vmem,
        ],
        out_specs=(vmem, vmem),
        scratch_shapes=[
            pltpu.VMEM((3 * channels, 3 * channels), jnp.bfloat16),
            pltpu.VMEM((points, channels), jnp.bfloat16),
            pltpu.VMEM((points // CHUNK, capacity, CHUNK), jnp.bfloat16),
            pltpu.VMEM((points, 128), jnp.bfloat16),
            pltpu.VMEM((points, 256), jnp.bfloat16),
            pltpu.VMEM((devices, capacity, channels), jnp.bfloat16),
            pltpu.VMEM((devices, 1, stride), jnp.float32),
            pltpu.VMEM((devices, capacity, channels), jnp.bfloat16),
            pltpu.VMEM((devices, 1, stride), jnp.float32),
            pltpu.VMEM((COLS_DEV, ROWS_DEV * channels), jnp.float32),
            pltpu.VMEM((ROWS_DEV + 2, COLS_DEV, channels), jnp.bfloat16),
            pltpu.VMEM((2, ROWS_DEV, 1, channels), jnp.float32),
            pltpu.VMEM((2, ROWS_DEV + 2, 1, channels), jnp.float32),
            pltpu.VMEM((2, ROWS_DEV, 1, channels), jnp.float32),
            pltpu.VMEM((2 * ROWS_DEV, channels), jnp.float32),
            dma((1,)),
            dma((devices,)),
            dma((devices,)),
            dma((devices,)),
            dma((devices,)),
            dma((2,)),
            dma((len(NEIGHBOURS),)),
            dma((len(NEIGHBOURS),)),
        ],
        compiler_params=pltpu.CompilerParams(
            collective_id=0, has_side_effects=True, vmem_limit_bytes=36 * 1024 * 1024
        ),
        name="make_map",
    )(count, feats, named, cell, weight, bias)


def shards(point_feats, point_tile, point_cell, point_count, conv_weight, conv_bias):
    size_gx = lax.axis_size("gx")
    size_gy = lax.axis_size("gy")
    devices = size_gx * size_gy
    points = point_feats.shape[0]
    channels = point_feats.shape[1]
    capacity = 5 * points // (4 * devices)
    return make_map(
        point_count,
        point_feats,
        point_tile.reshape(-1, 1, CHUNK),
        point_cell.reshape(-1, 1, CHUNK),
        conv_weight,
        conv_bias.reshape(1, channels),
        size_gx,
        size_gy,
        capacity,
    )


def solution(mesh):
    in_specs = (
        P(("gx", "gy"), None),
        P(("gx", "gy"), None),
        P(("gx", "gy")),
        P(("gx", "gy")),
        P(),
        P(),
    )
    out_specs = (P("gx", "gy", None), P("gx", "gy", None))
    return jax.shard_map(shards, mesh=mesh, in_specs=in_specs, out_specs=out_specs, check_vma=False)
```

```python
import functools

import jax
import jax.numpy as jnp
from jax import lax
from jax.experimental import pallas as pl
from jax.experimental.pallas import tpu as pltpu
from jax.sharding import PartitionSpec as P

COLS_DEV = 256
ROWS_DEV = 16
CELLS = ROWS_DEV * COLS_DEV


MESH = pl.DeviceIdType.MESH
GROUP = 4
CHUNK = 1024
NEIGHBOURS = [(dx, dy) for dx in (-1, 0, 1) for dy in (-1, 0, 1) if (dx, dy) != (0, 0)]


def map_kernel(
    size_gx,
    size_gy,
    count,
    source,
    all_named,
    all_cell,
    taps,
    all_bias,
    bev,
    conv,
    weight,
    feats,
    named,
    cell,
    bias,
    slots,
    tiles,
    marks,
    send_feats,
    send_cells,
    got_feats,
    got_cells,
    acc,
    pad,
    edges,
    sides,
    ends,
    flat,
    fetch,
    send_f,
    recv_f,
    send_c,
    recv_c,
    own,
    send_h,
    recv_h,
):
    devices = size_gx * size_gy
    capacity = send_feats.shape[1]
    gx, gy = lax.axis_index("gx"), lax.axis_index("gy")
    me = gx * size_gy + gy

    barrier = pltpu.get_barrier_semaphore()

    @pl.loop(1, devices)
    def _(k):
        other = lax.rem(me + k, devices)
        pl.semaphore_signal(
            barrier, inc=1, device_id=(other // size_gy, lax.rem(other, size_gy)), device_id_type=MESH
        )

    points = (
        pltpu.make_async_copy(all_named, named, fetch.at[0]),
        pltpu.make_async_copy(all_cell, cell, fetch.at[1]),
    )
    load = pltpu.make_async_copy(source, feats, fetch.at[2])
    later = [pltpu.make_async_copy(all_bias, bias, fetch.at[3])]
    for a in range(3):
        for b in range(3):
            block = weight.at[pl.ds(a * 128, 128), pl.ds(b * 128, 128)]
            later.append(pltpu.make_async_copy(taps.at[a, b], block, fetch.at[4 + a * 3 + b]))
    for copy in (*points, load, *later):
        copy.start()

    for r in (0, ROWS_DEV + 1):
        pad[r] = jnp.zeros_like(pad[r])
    sides[...] = jnp.zeros_like(sides)

    chunks = named.shape[0]

    inner = 256
    upper = lax.broadcasted_iota(jnp.int32, (inner, inner), 0) <= lax.broadcasted_iota(
        jnp.int32, (inner, inner), 1
    )
    upper = jnp.where(upper, 1.0, 0.0).astype(jnp.bfloat16)
    names = lax.broadcasted_iota(jnp.int32, (devices, inner), 0)

    width = marks.shape[1] // 2
    gap = jnp.zeros((width - devices, inner), jnp.float32)

    middle = capacity // 2
    assert middle < 256
    ids = lax.broadcasted_iota(jnp.int32, (capacity, CHUNK), 0) - middle
    ids = ids.astype(jnp.float32).astype(jnp.bfloat16)

    def prepare(c, before):
        slot = lax.broadcasted_iota(jnp.int32, (1, CHUNK), 1) + c * CHUNK
        target = jnp.where(slot < count[0], named[c], devices)
        row = jnp.right_shift(cell[c], 8).astype(jnp.float32) * 256.0
        col = (cell[c] & (COLS_DEV - 1)).astype(jnp.float32)
        hits = jnp.concatenate(
            [jnp.where(names == target[:, at : at + inner], 1.0, 0.0) for at in range(0, CHUNK, inner)],
            axis=0,
        )
        ranks = jnp.dot(hits.astype(jnp.bfloat16), upper, preferred_element_type=jnp.float32)
        found = []
        for k in range(CHUNK // inner):
            hit, rank = (x[k * devices : (k + 1) * devices] for x in (hits, ranks))
            found.append(jnp.sum(hit * (rank + before), axis=0, keepdims=True) - 1.0)
            before = before + rank[:, inner - 1 : inner]
            at = slice(k * inner, (k + 1) * inner)
            mark = [hit * row[:, at], gap, hit * col[:, at], gap]
            mark = jnp.concatenate([m for m in mark if m.shape[0]], axis=0)
            marks[c, :, at] = mark.astype(jnp.bfloat16)
        place = (jnp.concatenate(found, axis=1) - middle).astype(jnp.bfloat16)
        rows = pl.ds(c * CHUNK, CHUNK)
        slots[c] = jnp.where(ids == place, jnp.bfloat16(1), jnp.bfloat16(0))
        tile = jnp.transpose(jnp.broadcast_to(target.astype(jnp.float32), (128, CHUNK)))
        tiles[rows, :] = tile.astype(jnp.bfloat16)
        return before

    for copy in points:
        copy.wait()
    before = jnp.zeros((devices, inner), jnp.float32)
    for c in range(chunks):
        before = prepare(c, before)

    def packed(operand):
        total = None
        for c in range(chunks):
            part = jnp.dot(slots[c], operand(c), preferred_element_type=jnp.float32)
            total = part if total is None else total + part
        return total

    def copies(source, owner, target):
        where = dict(
            device_id=(target // size_gy, lax.rem(target, size_gy)), device_id_type=MESH
        )
        return (
            pltpu.make_async_remote_copy(
                send_cells.at[source], got_cells.at[owner],
                send_c.at[source], recv_c.at[owner], **where,
            ),
            pltpu.make_async_remote_copy(
                send_feats.at[source], got_feats.at[owner], send_f.at[source], recv_f.at[owner], **where
            ),
        )

    mine = (
        pltpu.make_async_copy(send_cells.at[me], got_cells.at[me], own.at[0]),
        pltpu.make_async_copy(send_feats.at[me], got_feats.at[me], own.at[1]),
    )
    pairs = devices // 2
    half = me // 2

    def offset(q):
        return lax.rem(2 * q + 1, pairs) - q // (pairs // 2)

    def pack(q):
        pair = lax.rem(half + offset(q), pairs)
        names = [(pair * 2 + k).astype(jnp.float32).astype(jnp.bfloat16) for k in range(2)]

        def masked(c):
            rows = slice(c * CHUNK, (c + 1) * CHUNK)
            values, tile = feats[rows, :], tiles[rows, :]
            zero = jnp.zeros_like(values)
            return jnp.concatenate([jnp.where(tile == n, values, zero) for n in names], axis=1)

        block = packed(masked).astype(jnp.bfloat16)
        for k in range(2):
            send_feats[pair * 2 + k] = block[:, k * 128 : (k + 1) * 128]

    def send(q, parts=(0, 1)):
        pair = lax.rem(half + offset(q), pairs)
        for k in range(2):
            target = pair * 2 + k

            @pl.when(target != me)
            def _():
                for part in parts:
                    copies(target, me, target)[part].start()

            @pl.when(target == me)
            def _():
                for part in parts:
                    mine[part].start()

    load.wait()
    pack(jnp.int32(0))

    found = None
    for c in range(chunks):
        part = lax.dot_general(
            slots[c], marks[c], (((1,), (1,)), ((), ())), preferred_element_type=jnp.float32
        )
        found = part if found is None else found + part
    if send_cells.shape[2] > capacity:
        extra = (send_cells.shape[2] - capacity, found.shape[1])
        found = jnp.concatenate([found, jnp.zeros(extra, jnp.float32)], axis=0)
    found = jnp.transpose(found)
    found = found[:devices] + found[width : width + devices]
    for t in range(devices):
        send_cells[t] = found[t : t + 1, :]

    pl.semaphore_wait(barrier, devices - 1)
    send(jnp.int32(0))


    @pl.loop(1, pairs)
    def _(q):
        pack(q)

        @pl.when(q > 1)
        def _():
            send(q - 1)

    for copy in later:
        copy.wait()
    send(jnp.int32(pairs - 1))
    acc[...] = jnp.zeros_like(acc)

    def receive(positions):
        owners = []
        for j in positions:
            q = lax.rem(j + pairs // 2, pairs)
            pair = lax.rem(half + pairs - offset(q), pairs)
            owners += [pair * 2, pair * 2 + 1]

        def arrived(part):
            for owner in owners:

                @pl.when(owner != me)
                def _():
                    copies(owner, owner, owner)[part].wait_recv()

                @pl.when(owner == me)
                def _():
                    mine[part].wait()

        arrived(0)
        row, col = [], []
        for owner in owners:
            part = got_cells[owner].astype(jnp.int32)
            at = jnp.right_shift(part, 8).astype(jnp.float32)
            at = jnp.transpose(jnp.broadcast_to(at, (128, part.shape[1])))
            row.append(at[:capacity].astype(jnp.bfloat16))
            col.append(part[:, :capacity] & (COLS_DEV - 1))
        row = jnp.concatenate(row, axis=0)
        col = jnp.concatenate(col, axis=1)
        ids = lax.broadcasted_iota(jnp.int32, (COLS_DEV, col.shape[1]), 0)
        onehot = jnp.where(ids == col, 1.0, 0.0).astype(jnp.bfloat16)
        arrived(1)
        values = jnp.concatenate([got_feats[owner] for owner in owners], axis=0)
        zero = jnp.zeros_like(values)

        def added(rows):
            masked = jnp.concatenate(
                [jnp.where(row == jnp.bfloat16(r), values, zero) for r in rows], axis=1
            )
            return jnp.dot(onehot, masked, preferred_element_type=jnp.float32)

        return added

    group = GROUP // 2

    @pl.loop(0, pairs // group - 1)
    def _(g):
        added = receive([g * group + j for j in range(group)])
        for r in range(0, ROWS_DEV, 2):
            acc[:, r * 128 : (r + 2) * 128] += added((r, r + 1))

    for j in range(pairs - group, pairs - 1):
        added = receive([jnp.int32(j)])
        for r in range(0, ROWS_DEV, 2):
            acc[:, r * 128 : (r + 2) * 128] += added((r, r + 1))

    def inside(x, y):
        return (x >= 0) & (x < size_gx) & (y >= 0) & (y < size_gy)

    def halo(i):
        dx, dy = NEIGHBOURS[i]
        if dy == 0:
            src, dst = (pad.at[1], pad.at[ROWS_DEV + 1]) if dx < 0 else (pad.at[ROWS_DEV], pad.at[0])
        else:
            from_side, to_side = (0, 1) if dy < 0 else (1, 0)
            if dx == 0:
                src = edges.at[from_side]
                dst = sides.at[to_side, pl.ds(1, ROWS_DEV)]
            else:
                at = 0 if dx < 0 else ROWS_DEV - 1
                src = edges.at[from_side, pl.ds(at, 1)]
                dst = sides.at[to_side, pl.ds(ROWS_DEV + 1 if dx < 0 else 0, 1)]
        return pltpu.make_async_remote_copy(
            src, dst, send_h.at[i], recv_h.at[i], device_id=(gx + dx, gy + dy), device_id_type=MESH
        )

    def start(which):
        for i, (dx, dy) in enumerate(NEIGHBOURS):
            if which(dx, dy):

                @pl.when(inside(gx + dx, gy + dy))
                def _():
                    halo(i).start()

    added = receive([jnp.int32(pairs - 1)])
    order = [(0, ROWS_DEV - 1)] + [(r, r + 1) for r in range(1, ROWS_DEV - 1, 2)]
    for step, rows in enumerate(order):
        part = added(rows)
        for k, r in enumerate(rows):
            total = acc[:, r * 128 : (r + 1) * 128] + part[:, k * 128 : (k + 1) * 128]
            cells = total.astype(jnp.bfloat16)
            pad[r + 1] = cells
            bev[r] = cells
            for side, c in ((0, 0), (1, COLS_DEV - 1)):
                edges[side, r] = total[c : c + 1].astype(jnp.bfloat16).astype(jnp.float32)
        if step == 1:
            start(lambda dx, dy: dy == 0)
        if step == 2:
            start(lambda dx, dy: dx != 0 and dy != 0)

    place = lax.broadcasted_iota(jnp.int32, (COLS_DEV, 128), 0)

    def sums_of(r):
        near = jnp.concatenate([pad[r + a] for a in range(3)], axis=1)
        sums = jnp.dot(near, weight[...], preferred_element_type=jnp.float32)
        left = jnp.where(place == 0, 0.0, pltpu.roll(sums[:, :128], 1, 0))
        right = jnp.where(place == COLS_DEV - 1, 0.0, pltpu.roll(sums[:, 256:], COLS_DEV - 1, 0))
        total = sums[:, 128:256] + left + right + bias[...]
        for side, c in ((0, 0), (1, COLS_DEV - 1)):
            ends[side, r] = total[c : c + 1]
        conv[r] = jnp.maximum(total, 0.0).astype(jnp.bfloat16)

    start(lambda dx, dy: dx == 0)

    @pl.loop(1, ROWS_DEV - 1)
    def _(r):
        sums_of(r)

    for i, (dx, dy) in enumerate(NEIGHBOURS):

        @pl.when(inside(gx - dx, gy - dy))
        def _():
            halo(i).wait_recv()

    for r in (0, ROWS_DEV - 1):
        sums_of(r)

    side_sums = []
    for side in range(2):
        for r in range(ROWS_DEV + 2):
            flat[r : r + 1, :] = sides[side, r]
        near = jnp.concatenate([flat[a : a + ROWS_DEV, :] for a in range(3)], axis=1)
        part = weight[:, :128] if side == 0 else weight[:, 256:]
        side_sums.append(
            jnp.dot(near.astype(jnp.bfloat16), part, preferred_element_type=jnp.float32)
        )
    lines = 16
    place = lax.broadcasted_iota(jnp.int32, (lines, 128), 0)
    for side, c in ((0, 0), (1, COLS_DEV - 1)):
        rows = pl.ds(c // lines * lines, lines)
        for r in range(ROWS_DEV):
            total = jnp.maximum(ends[side, r] + side_sums[side][r : r + 1], 0.0)
            kept = conv[r, rows, :].astype(jnp.float32)
            conv[r, rows, :] = jnp.where(place == c % lines, total, kept).astype(jnp.bfloat16)

    for i, (dx, dy) in enumerate(NEIGHBOURS):

        @pl.when(inside(gx + dx, gy + dy))
        def _():
            halo(i).wait_send()

    @pl.loop(1, devices)
    def _(k):
        other = lax.rem(me + k, devices)
        for copy in copies(other, me, other):
            copy.wait_send()


def make_map(count, feats, named, cell, weight, bias, size_gx, size_gy, capacity):
    devices = size_gx * size_gy
    points, channels = feats.shape
    stride = -(-capacity // 128) * 128
    vmem = pl.BlockSpec(memory_space=pltpu.VMEM)
    shape = pltpu.VMEM((ROWS_DEV, COLS_DEV, channels), jnp.bfloat16)
    hbm = [
        pltpu.with_memory_space_constraint(a, pltpu.HBM)
        for a in (feats, named, cell, weight, bias)
    ]
    dma = pltpu.SemaphoreType.DMA
    return pl.pallas_call(
        functools.partial(map_kernel, size_gx, size_gy),
        out_shape=(shape, shape),
        in_specs=[
            pl.BlockSpec(memory_space=pltpu.SMEM),
            *[pl.BlockSpec(memory_space=pltpu.HBM)] * len(hbm),
        ],
        out_specs=(vmem, vmem),
        scratch_shapes=[
            pltpu.VMEM((3 * channels, 3 * channels), jnp.bfloat16),
            pltpu.VMEM((points, channels), jnp.bfloat16),
            pltpu.VMEM(named.shape, jnp.int32),
            pltpu.VMEM(cell.shape, jnp.int32),
            pltpu.VMEM(bias.shape, jnp.float32),
            pltpu.VMEM((points // CHUNK, capacity, CHUNK), jnp.bfloat16),
            pltpu.VMEM((points, 128), jnp.bfloat16),
            pltpu.VMEM((points // CHUNK, 2 * max(devices, 64), CHUNK), jnp.bfloat16),
            pltpu.VMEM((devices, capacity, channels), jnp.bfloat16),
            pltpu.VMEM((devices, 1, stride), jnp.float32),
            pltpu.VMEM((devices, capacity, channels), jnp.bfloat16),
            pltpu.VMEM((devices, 1, stride), jnp.float32),
            pltpu.VMEM((COLS_DEV, ROWS_DEV * channels), jnp.float32),
            pltpu.VMEM((ROWS_DEV + 2, COLS_DEV, channels), jnp.bfloat16),
            pltpu.VMEM((2, ROWS_DEV, 1, channels), jnp.float32),
            pltpu.VMEM((2, ROWS_DEV + 2, 1, channels), jnp.float32),
            pltpu.VMEM((2, ROWS_DEV, 1, channels), jnp.float32),
            pltpu.VMEM((2 * ROWS_DEV, channels), jnp.float32),
            dma((13,)),
            dma((devices,)),
            dma((devices,)),
            dma((devices,)),
            dma((devices,)),
            dma((2,)),
            dma((len(NEIGHBOURS),)),
            dma((len(NEIGHBOURS),)),
        ],
        compiler_params=pltpu.CompilerParams(
            collective_id=0, has_side_effects=True, vmem_limit_bytes=36 * 1024 * 1024
        ),
        name="make_map",
    )(count, *hbm)


def shards(point_feats, point_tile, point_cell, point_count, conv_weight, conv_bias):
    size_gx = lax.axis_size("gx")
    size_gy = lax.axis_size("gy")
    devices = size_gx * size_gy
    points = point_feats.shape[0]
    channels = point_feats.shape[1]
    capacity = 5 * points // (4 * devices)
    return make_map(
        point_count,
        point_feats,
        point_tile.reshape(-1, 1, CHUNK),
        point_cell.reshape(-1, 1, CHUNK),
        conv_weight,
        conv_bias.reshape(1, channels),
        size_gx,
        size_gy,
        capacity,
    )


def solution(mesh):
    in_specs = (
        P(("gx", "gy"), None),
        P(("gx", "gy"), None),
        P(("gx", "gy")),
        P(("gx", "gy")),
        P(),
        P(),
    )
    out_specs = (P("gx", "gy", None), P("gx", "gy", None))
    return jax.shard_map(shards, mesh=mesh, in_specs=in_specs, out_specs=out_specs, check_vma=False)
```

```python
import functools

import jax
import jax.numpy as jnp
from jax import lax
from jax.experimental import pallas as pl
from jax.experimental.pallas import tpu as pltpu
from jax.sharding import PartitionSpec as P

COLS_DEV = 256
ROWS_DEV = 16
CELLS = ROWS_DEV * COLS_DEV


MESH = pl.DeviceIdType.MESH
GROUP = 4
CHUNK = 1024
NEIGHBOURS = [(dx, dy) for dx in (-1, 0, 1) for dy in (-1, 0, 1) if (dx, dy) != (0, 0)]


def map_kernel(
    size_gx,
    size_gy,
    count,
    source,
    all_named,
    all_cell,
    taps,
    all_bias,
    bev,
    conv,
    weight,
    feats,
    named,
    cell,
    bias,
    slots,
    tiles,
    marks,
    send_feats,
    send_cells,
    got_feats,
    got_cells,
    send_map,
    got_map,
    acc,
    pad,
    edges,
    sides,
    ends,
    flat,
    fetch,
    send_f,
    recv_f,
    send_c,
    recv_c,
    own,
    send_h,
    recv_h,
    send_d,
    recv_d,
):
    devices = size_gx * size_gy
    capacity = send_feats.shape[1]
    gx, gy = lax.axis_index("gx"), lax.axis_index("gy")
    me = gx * size_gy + gy

    barrier = pltpu.get_barrier_semaphore()

    @pl.loop(1, devices)
    def _(k):
        peer = lax.rem(me + k, devices)
        pl.semaphore_signal(
            barrier, inc=1, device_id=(peer // size_gy, lax.rem(peer, size_gy)), device_id_type=MESH
        )

    points = (
        pltpu.make_async_copy(all_named, named, fetch.at[0]),
        pltpu.make_async_copy(all_cell, cell, fetch.at[1]),
    )
    load = pltpu.make_async_copy(source, feats, fetch.at[2])
    later = [pltpu.make_async_copy(all_bias, bias, fetch.at[3])]
    for a in range(3):
        for b in range(3):
            block = weight.at[pl.ds(a * 128, 128), pl.ds(b * 128, 128)]
            later.append(pltpu.make_async_copy(taps.at[a, b], block, fetch.at[4 + a * 3 + b]))
    for copy in (*points, load, *later):
        copy.start()

    for r in (0, ROWS_DEV + 1):
        pad[r] = jnp.zeros_like(pad[r])
    sides[...] = jnp.zeros_like(sides)

    chunks = named.shape[0]

    inner = 256
    upper = lax.broadcasted_iota(jnp.int32, (inner, inner), 0) <= lax.broadcasted_iota(
        jnp.int32, (inner, inner), 1
    )
    upper = jnp.where(upper, 1.0, 0.0).astype(jnp.bfloat16)
    names = lax.broadcasted_iota(jnp.int32, (devices, inner), 0)

    width = marks.shape[1] // 2
    gap = jnp.zeros((width - devices, inner), jnp.float32)

    middle = capacity // 2
    assert middle < 256
    ids = lax.broadcasted_iota(jnp.int32, (capacity, CHUNK), 0) - middle
    ids = ids.astype(jnp.float32).astype(jnp.bfloat16)

    def prepare(c, before):
        slot = lax.broadcasted_iota(jnp.int32, (1, CHUNK), 1) + c * CHUNK
        target = jnp.where(slot < count[0], named[c], devices)
        row = jnp.right_shift(cell[c], 8).astype(jnp.float32) * 256.0
        col = (cell[c] & (COLS_DEV - 1)).astype(jnp.float32)
        hits = jnp.concatenate(
            [jnp.where(names == target[:, at : at + inner], 1.0, 0.0) for at in range(0, CHUNK, inner)],
            axis=0,
        )
        ranks = jnp.dot(hits.astype(jnp.bfloat16), upper, preferred_element_type=jnp.float32)
        found = []
        for k in range(CHUNK // inner):
            hit, rank = (x[k * devices : (k + 1) * devices] for x in (hits, ranks))
            found.append(jnp.sum(hit * (rank + before), axis=0, keepdims=True) - 1.0)
            before = before + rank[:, inner - 1 : inner]
            at = slice(k * inner, (k + 1) * inner)
            mark = [hit * row[:, at], gap, hit * col[:, at], gap]
            mark = jnp.concatenate([m for m in mark if m.shape[0]], axis=0)
            marks[c, :, at] = mark.astype(jnp.bfloat16)
        place = (jnp.concatenate(found, axis=1) - middle).astype(jnp.bfloat16)
        rows = pl.ds(c * CHUNK, CHUNK)
        slots[c] = jnp.where(ids == place, jnp.bfloat16(1), jnp.bfloat16(0))
        tile = jnp.transpose(jnp.broadcast_to(target.astype(jnp.float32), (128, CHUNK)))
        tiles[rows, :] = tile.astype(jnp.bfloat16)
        return before

    for copy in points:
        copy.wait()
    before = jnp.zeros((devices, inner), jnp.float32)
    for c in range(chunks):
        before = prepare(c, before)

    def packed(operand):
        total = None
        for c in range(chunks):
            part = jnp.dot(slots[c], operand(c), preferred_element_type=jnp.float32)
            total = part if total is None else total + part
        return total

    pairs = devices // 2
    half = pairs // 2
    quarter = size_gy // 4
    upper_me = gy >= size_gy // 2

    def between(y):
        return (y >= quarter) & (y < size_gy - quarter)

    def mirror(y):
        return size_gy - 1 - y

    dense = between(gy)
    other = gx * size_gy + mirror(gy)

    def pair_at(q, sign):
        i = lax.rem(q, half)
        far = (q < half) != upper_me
        col = lax.rem(gx + sign * (i // quarter) + size_gx, size_gx)
        line = lax.rem(lax.rem(gy // 2, quarter) + sign * lax.rem(i, quarter) + quarter, quarter)
        return col * (2 * quarter) + jnp.where(far, quarter, 0) + line

    def route(tile):
        x, y = tile // size_gy, lax.rem(tile, size_gy)
        relay = between(y) & ((y >= size_gy // 2) != upper_me)
        target = x * size_gy + jnp.where(relay, mirror(y), y)
        return target, jnp.where(relay, other, me)

    def copies(source, slot, target):
        where = dict(
            device_id=(target // size_gy, lax.rem(target, size_gy)), device_id_type=MESH
        )
        return (
            pltpu.make_async_remote_copy(
                send_cells.at[source], got_cells.at[slot],
                send_c.at[source], recv_c.at[slot], **where,
            ),
            pltpu.make_async_remote_copy(
                send_feats.at[source], got_feats.at[slot], send_f.at[source], recv_f.at[slot], **where
            ),
        )

    def mine(slot):
        at = jnp.where(slot == me, 0, 2)
        return (
            pltpu.make_async_copy(send_cells.at[slot], got_cells.at[slot], own.at[at]),
            pltpu.make_async_copy(send_feats.at[slot], got_feats.at[slot], own.at[at + 1]),
        )

    def pack(q):
        pair = pair_at(q, 1)
        names = [(pair * 2 + k).astype(jnp.float32).astype(jnp.bfloat16) for k in range(2)]

        def masked(c):
            rows = slice(c * CHUNK, (c + 1) * CHUNK)
            values, tile = feats[rows, :], tiles[rows, :]
            zero = jnp.zeros_like(values)
            return jnp.concatenate([jnp.where(tile == n, values, zero) for n in names], axis=1)

        block = packed(masked).astype(jnp.bfloat16)
        for k in range(2):
            send_feats[pair * 2 + k] = block[:, k * 128 : (k + 1) * 128]

    def send(q):
        pair = pair_at(q, 1)
        for k in range(2):
            tile = pair * 2 + k
            target, slot = route(tile)

            @pl.when(target != me)
            def _():
                for copy in copies(tile, slot, target):
                    copy.start()

            @pl.when(target == me)
            def _():
                for copy in mine(tile):
                    copy.start()

    load.wait()
    pack(jnp.int32(0))

    found = None
    for c in range(chunks):
        part = lax.dot_general(
            slots[c], marks[c], (((1,), (1,)), ((), ())), preferred_element_type=jnp.float32
        )
        found = part if found is None else found + part
    if send_cells.shape[2] > capacity:
        extra = (send_cells.shape[2] - capacity, found.shape[1])
        found = jnp.concatenate([found, jnp.zeros(extra, jnp.float32)], axis=0)
    found = jnp.transpose(found)
    found = found[:devices] + found[width : width + devices]
    for t in range(devices):
        send_cells[t] = found[t : t + 1, :]

    pl.semaphore_wait(barrier, devices - 1)
    send(jnp.int32(0))

    acc[...] = jnp.zeros_like(acc)

    def advance(q):
        pack(q)

        @pl.when(q > 1)
        def _():
            send(q - 1)

    turn = half + half // 2

    @pl.loop(1, turn)
    def _(q):
        advance(q)

    def receive(positions):
        owners = []
        for j in positions:
            pair = pair_at(j, -1)
            owners += [pair * 2, pair * 2 + 1]

        def arrived(part):
            for owner in owners:
                local = (owner == me) | (dense & (owner == other))

                @pl.when(jnp.logical_not(local))
                def _():
                    copies(owner, owner, owner)[part].wait_recv()

                @pl.when(local)
                def _():
                    mine(owner)[part].wait()

        arrived(0)
        row, col = [], []
        for owner in owners:
            part = got_cells[owner].astype(jnp.int32)
            at = jnp.right_shift(part, 8).astype(jnp.float32)
            at = jnp.transpose(jnp.broadcast_to(at, (128, part.shape[1])))
            row.append(at[:capacity].astype(jnp.bfloat16))
            col.append(part[:, :capacity] & (COLS_DEV - 1))
        row = jnp.concatenate(row, axis=0)
        col = jnp.concatenate(col, axis=1)
        ids = lax.broadcasted_iota(jnp.int32, (COLS_DEV, col.shape[1]), 0)
        onehot = jnp.where(ids == col, 1.0, 0.0).astype(jnp.bfloat16)
        arrived(1)
        values = jnp.concatenate([got_feats[owner] for owner in owners], axis=0)
        zero = jnp.zeros_like(values)

        def added(rows):
            masked = jnp.concatenate(
                [jnp.where(row == jnp.bfloat16(r), values, zero) for r in rows], axis=1
            )
            return jnp.dot(onehot, masked, preferred_element_type=jnp.float32)

        return added

    group = GROUP // 2

    def gather(first):
        @pl.loop(0, half // group)
        def _(g):
            added = receive([first + g * group + j for j in range(group)])
            for r in range(0, ROWS_DEV, 2):
                acc[:, r * 128 : (r + 2) * 128] += added((r, r + 1))

    order = [(0, ROWS_DEV - 1)] + [(r, r + 1) for r in range(1, ROWS_DEV - 1, 2)]

    def partial(r):
        return pltpu.make_async_remote_copy(
            send_map.at[r], got_map.at[r], send_d.at[r], recv_d.at[r],
            device_id=(gx, mirror(gy)), device_id_type=MESH,
        )

    @pl.when(dense)
    def _():
        gather(0)
        before = ()
        for rows in order:
            for r in rows:
                send_map[r] = acc[:, r * 128 : (r + 1) * 128].astype(jnp.bfloat16)
            for r in before:
                partial(r).start()
            before = rows
        acc[...] = jnp.zeros_like(acc)
        for r in before:
            partial(r).start()

    @pl.when(jnp.logical_not(dense))
    def _():
        got_map[...] = jnp.zeros_like(got_map)

    @pl.loop(turn, pairs)
    def _(q):
        advance(q)

    send(jnp.int32(pairs - 1))
    for copy in later:
        copy.wait()
    gather(half)

    @pl.when(jnp.logical_not(dense))
    def _():
        gather(0)

    def inside(x, y):
        return (x >= 0) & (x < size_gx) & (y >= 0) & (y < size_gy)

    def halo(i):
        dx, dy = NEIGHBOURS[i]
        if dy == 0:
            src, dst = (pad.at[1], pad.at[ROWS_DEV + 1]) if dx < 0 else (pad.at[ROWS_DEV], pad.at[0])
        else:
            from_side, to_side = (0, 1) if dy < 0 else (1, 0)
            if dx == 0:
                src = edges.at[from_side]
                dst = sides.at[to_side, pl.ds(1, ROWS_DEV)]
            else:
                at = 0 if dx < 0 else ROWS_DEV - 1
                src = edges.at[from_side, pl.ds(at, 1)]
                dst = sides.at[to_side, pl.ds(ROWS_DEV + 1 if dx < 0 else 0, 1)]
        return pltpu.make_async_remote_copy(
            src, dst, send_h.at[i], recv_h.at[i], device_id=(gx + dx, gy + dy), device_id_type=MESH
        )

    def start(which):
        for i, (dx, dy) in enumerate(NEIGHBOURS):
            if which(dx, dy):

                @pl.when(inside(gx + dx, gy + dy))
                def _():
                    halo(i).start()

    for step, rows in enumerate(order):
        for r in rows:

            @pl.when(dense)
            def _():
                partial(r).wait_recv()

            total = acc[:, r * 128 : (r + 1) * 128] + got_map[r].astype(jnp.float32)
            cells = total.astype(jnp.bfloat16)
            pad[r + 1] = cells
            bev[r] = cells
            for side, c in ((0, 0), (1, COLS_DEV - 1)):
                edges[side, r] = total[c : c + 1].astype(jnp.bfloat16).astype(jnp.float32)
        if step == 1:
            start(lambda dx, dy: dy == 0)
        if step == 2:
            start(lambda dx, dy: dx != 0 and dy != 0)

    place = lax.broadcasted_iota(jnp.int32, (COLS_DEV, 128), 0)

    def sums_of(r):
        near = jnp.concatenate([pad[r + a] for a in range(3)], axis=1)
        sums = jnp.dot(near, weight[...], preferred_element_type=jnp.float32)
        left = jnp.where(place == 0, 0.0, pltpu.roll(sums[:, :128], 1, 0))
        right = jnp.where(place == COLS_DEV - 1, 0.0, pltpu.roll(sums[:, 256:], COLS_DEV - 1, 0))
        total = sums[:, 128:256] + left + right + bias[...]
        for side, c in ((0, 0), (1, COLS_DEV - 1)):
            ends[side, r] = total[c : c + 1]
        conv[r] = jnp.maximum(total, 0.0).astype(jnp.bfloat16)

    start(lambda dx, dy: dx == 0)

    @pl.loop(1, ROWS_DEV - 1)
    def _(r):
        sums_of(r)

    for i, (dx, dy) in enumerate(NEIGHBOURS):

        @pl.when(inside(gx - dx, gy - dy))
        def _():
            halo(i).wait_recv()

    for r in (0, ROWS_DEV - 1):
        sums_of(r)

    side_sums = []
    for side in range(2):
        for r in range(ROWS_DEV + 2):
            flat[r : r + 1, :] = sides[side, r]
        near = jnp.concatenate([flat[a : a + ROWS_DEV, :] for a in range(3)], axis=1)
        part = weight[:, :128] if side == 0 else weight[:, 256:]
        side_sums.append(
            jnp.dot(near.astype(jnp.bfloat16), part, preferred_element_type=jnp.float32)
        )
    lines = 16
    place = lax.broadcasted_iota(jnp.int32, (lines, 128), 0)
    for side, c in ((0, 0), (1, COLS_DEV - 1)):
        rows = pl.ds(c // lines * lines, lines)
        for r in range(ROWS_DEV):
            total = jnp.maximum(ends[side, r] + side_sums[side][r : r + 1], 0.0)
            kept = conv[r, rows, :].astype(jnp.float32)
            conv[r, rows, :] = jnp.where(place == c % lines, total, kept).astype(jnp.bfloat16)

    for i, (dx, dy) in enumerate(NEIGHBOURS):

        @pl.when(inside(gx + dx, gy + dy))
        def _():
            halo(i).wait_send()

    @pl.when(dense)
    def _():
        for r in range(ROWS_DEV):
            partial(r).wait_send()

    @pl.loop(0, devices)
    def _(tile):
        target, slot = route(tile)

        @pl.when(target != me)
        def _():
            for copy in copies(tile, slot, target):
                copy.wait_send()


def make_map(count, feats, named, cell, weight, bias, size_gx, size_gy, capacity):
    devices = size_gx * size_gy
    points, channels = feats.shape
    stride = -(-capacity // 128) * 128
    vmem = pl.BlockSpec(memory_space=pltpu.VMEM)
    shape = pltpu.VMEM((ROWS_DEV, COLS_DEV, channels), jnp.bfloat16)
    hbm = [
        pltpu.with_memory_space_constraint(a, pltpu.HBM)
        for a in (feats, named, cell, weight, bias)
    ]
    dma = pltpu.SemaphoreType.DMA
    return pl.pallas_call(
        functools.partial(map_kernel, size_gx, size_gy),
        out_shape=(shape, shape),
        in_specs=[
            pl.BlockSpec(memory_space=pltpu.SMEM),
            *[pl.BlockSpec(memory_space=pltpu.HBM)] * len(hbm),
        ],
        out_specs=(vmem, vmem),
        scratch_shapes=[
            pltpu.VMEM((3 * channels, 3 * channels), jnp.bfloat16),
            pltpu.VMEM((points, channels), jnp.bfloat16),
            pltpu.VMEM(named.shape, jnp.int32),
            pltpu.VMEM(cell.shape, jnp.int32),
            pltpu.VMEM(bias.shape, jnp.float32),
            pltpu.VMEM((points // CHUNK, capacity, CHUNK), jnp.bfloat16),
            pltpu.VMEM((points, 128), jnp.bfloat16),
            pltpu.VMEM((points // CHUNK, 2 * max(devices, 64), CHUNK), jnp.bfloat16),
            pltpu.VMEM((devices, capacity, channels), jnp.bfloat16),
            pltpu.VMEM((devices, 1, stride), jnp.float32),
            pltpu.VMEM((devices, capacity, channels), jnp.bfloat16),
            pltpu.VMEM((devices, 1, stride), jnp.float32),
            pltpu.VMEM((ROWS_DEV, COLS_DEV, channels), jnp.bfloat16),
            pltpu.VMEM((ROWS_DEV, COLS_DEV, channels), jnp.bfloat16),
            pltpu.VMEM((COLS_DEV, ROWS_DEV * channels), jnp.float32),
            pltpu.VMEM((ROWS_DEV + 2, COLS_DEV, channels), jnp.bfloat16),
            pltpu.VMEM((2, ROWS_DEV, 1, channels), jnp.float32),
            pltpu.VMEM((2, ROWS_DEV + 2, 1, channels), jnp.float32),
            pltpu.VMEM((2, ROWS_DEV, 1, channels), jnp.float32),
            pltpu.VMEM((2 * ROWS_DEV, channels), jnp.float32),
            dma((13,)),
            dma((devices,)),
            dma((devices,)),
            dma((devices,)),
            dma((devices,)),
            dma((4,)),
            dma((len(NEIGHBOURS),)),
            dma((len(NEIGHBOURS),)),
            dma((ROWS_DEV,)),
            dma((ROWS_DEV,)),
        ],
        compiler_params=pltpu.CompilerParams(
            collective_id=0, has_side_effects=True, vmem_limit_bytes=36 * 1024 * 1024
        ),
        name="make_map",
    )(count, *hbm)


def shards(point_feats, point_tile, point_cell, point_count, conv_weight, conv_bias):
    size_gx = lax.axis_size("gx")
    size_gy = lax.axis_size("gy")
    devices = size_gx * size_gy
    points = point_feats.shape[0]
    channels = point_feats.shape[1]
    capacity = 5 * points // (4 * devices)
    return make_map(
        point_count,
        point_feats,
        point_tile.reshape(-1, 1, CHUNK),
        point_cell.reshape(-1, 1, CHUNK),
        conv_weight,
        conv_bias.reshape(1, channels),
        size_gx,
        size_gy,
        capacity,
    )


def solution(mesh):
    in_specs = (
        P(("gx", "gy"), None),
        P(("gx", "gy"), None),
        P(("gx", "gy")),
        P(("gx", "gy")),
        P(),
        P(),
    )
    out_specs = (P("gx", "gy", None), P("gx", "gy", None))
    return jax.shard_map(shards, mesh=mesh, in_specs=in_specs, out_specs=out_specs, check_vma=False)
```
